16 devices in a mesh: stage: 4 (over z, y), tp: 4 (over x, core).
Axes of the slice: x: 2, y: 2, z: 2, core: 2. Of those that a mesh axis runs over, the one named last changes fastest.
Arguments:
- x: bfloat16 [8, 1024, 2560], P(None, 'tp')
- g: bfloat16 [4, 2, 2560], P('stage')
- w1: bfloat16 [4, 2, 2560, 10240], P('stage', None, None, 'tp')
- w2: bfloat16 [4, 2, 10240, 2560], P('stage', None, 'tp')
Outputs:
- output: bfloat16 [4, 8, 1024, 2560], P('stage', None, 'tp')
All inputs are finite; a program needn't handle non-finite values.
Results may differ from the reference program's by a relative error of at most 0.02.
Values are sent between devices in bfloat16 or wider.
A program may use at most 1 GiB of HBM per device.

```python
import jax
import jax.numpy as jnp
from jax import lax

STAGES = 4
BLOCKS = 2
M = 8
T = 1024
D = 2560
FF = 10240

EPS = 1e-5


def setup_inputs(seed: int = 0) -> dict:
    k = jax.random.split(jax.random.key(seed), 4)
    x = jax.random.normal(k[0], (M, T, D), jnp.float32)
    g = 1.0 + 0.2 * jax.random.normal(k[1], (STAGES, BLOCKS, D), jnp.float32)
    w1 = jax.random.normal(k[2], (STAGES, BLOCKS, D, FF), jnp.float32) * D ** -0.5
    w2 = jax.random.normal(k[3], (STAGES, BLOCKS, FF, D), jnp.float32) * FF ** -0.5
    return {'x': x.astype(jnp.bfloat16), 'g': g.astype(jnp.bfloat16),
            'w1': w1.astype(jnp.bfloat16), 'w2': w2.astype(jnp.bfloat16)}


def _block(y, g, w1, w2):
    yf = y.astype(jnp.float32)
    mu = jnp.mean(yf, axis=-1, keepdims=True)
    var = jnp.mean(jnp.square(yf - mu), axis=-1, keepdims=True)
    h = ((yf - mu) * lax.rsqrt(var + EPS) * g.astype(jnp.float32)).astype(jnp.bfloat16)
    a = jax.nn.gelu(jnp.dot(h, w1, preferred_element_type=jnp.float32)).astype(jnp.bfloat16)
    return (yf + jnp.dot(a, w2, preferred_element_type=jnp.float32)).astype(jnp.bfloat16)


def reference(x, g, w1, w2):
    def one(xm):
        y = xm
        outs = []
        for s in range(STAGES):
            for b in range(BLOCKS):
                y = _block(y, g[s, b], w1[s, b], w2[s, b])
            outs.append(y)
        return jnp.stack(outs)
    return jnp.transpose(lax.map(one, x), (1, 0, 2, 3))
```

```python
import functools

import jax
import jax.numpy as jnp
from jax import lax
from jax.experimental import pallas as pl
from jax.experimental.pallas import tpu as pltpu
from jax.sharding import PartitionSpec as P

EPS = 1e-5
Q = 64
TN = 512
YS = 4
RB = 16
MESH = pl.DeviceIdType.MESH


def _kernel(cfg, x_hbm, g_ref, w1_hbm, w2_hbm, y_hbm,
            w1s, w2s, h, a, psend, precv, crossp, own, ssend, srecv, y0, y1, yout,
            w_sem, agp_send, agx_send, fw_send, ag_recv, p_send, p_recv, s_send, s_recv,
            yin_sem, ysend_sem, yhbm_sem, credit):
    S, NB, C, NQ, NT1, NT2, D = cfg
    q = Q
    n = 4 * q
    s = lax.axis_index('stage')
    r = lax.axis_index('tp')
    xr = lax.div(r, 2)
    cr = lax.rem(r, 2)
    partner = xr * 2 + (1 - cr)
    cross = (1 - xr) * 2 + cr

    def rows(i, k=1):
        return pl.ds(i * q, k * q)

    def w1_copy(b, t):
        return pltpu.make_async_copy(w1_hbm.at[b, :, pl.ds(t * TN, TN)], w1s.at[b, t], w_sem.at[0, b, t])

    def w2_copy(b, t):
        return pltpu.make_async_copy(w2_hbm.at[b, :, pl.ds(t * TN, TN)], w2s.at[b, t], w_sem.at[1, b, t])

    def remote(src, dst, ss, rs, **dev):
        return pltpu.make_async_remote_copy(src_ref=src, dst_ref=dst, send_sem=ss, recv_sem=rs,
                                            device_id=dev, device_id_type=MESH)

    def ag_partner(k):
        i = lax.rem(k, 3)
        return remote(h.at[i, rows(0)], h.at[i, rows(2)], agp_send.at[i], ag_recv.at[i, 1], tp=partner)

    def ag_cross(k):
        i = lax.rem(k, 3)
        return remote(h.at[i, rows(0)], h.at[i, rows(1)], agx_send.at[i], ag_recv.at[i, 0], tp=cross)

    def ag_forward(k):
        i = lax.rem(k, 3)
        return remote(h.at[i, rows(1)], h.at[i, rows(3)], fw_send.at[i], ag_recv.at[i, 2], tp=partner)

    def p_copy(k, t):
        return remote(psend.at[t % 2], precv.at[lax.rem(k, 2), t], p_send.at[t % 2],
                      p_recv.at[lax.rem(k, 2), t], tp=partner)

    def s_copy(k, t):
        return remote(ssend.at[lax.rem(k, 2), t], srecv.at[lax.rem(k, 3), t],
                      s_send.at[lax.rem(k, 2), t], s_recv.at[lax.rem(k, 3), t], tp=cross)

    def hbm_rows(ref, c):
        return ref.at[lax.div(c, NQ), pl.ds(pl.multiple_of(lax.rem(c, NQ) * q, q), q)]

    def x_copy(c):
        i = lax.rem(c, YS)
        return pltpu.make_async_copy(hbm_rows(x_hbm, c), y0.at[i], yin_sem.at[i])

    def y_next(c):
        i = lax.rem(c, YS)
        o = lax.rem(c, 2)
        return remote(yout.at[o], y0.at[i], ysend_sem.at[o], yin_sem.at[i], stage=s + 1)

    def y_store(c):
        o = lax.rem(c, 2)
        return pltpu.make_async_copy(yout.at[o], hbm_rows(y_hbm, c), yhbm_sem.at[o])

    def norm(yf, b):
        mu = jnp.mean(yf, axis=-1, keepdims=True)
        d = yf - mu
        var = jnp.mean(jnp.square(d), axis=-1, keepdims=True)
        return (d * lax.rsqrt(var + EPS) * g_ref[b]).astype(jnp.bfloat16)

    def send_h(k):
        ag_cross(k).start()
        ag_partner(k).start()

    def enter(c, k):
        i = lax.rem(c, YS)

        @pl.when(s == 0)
        def _():
            x_copy(c).wait()

            @pl.when(c + 2 < C)
            def _():
                x_copy(c + 2).start()

        @pl.when(s > 0)
        def _():
            y_next(c).wait_recv()

        def body(u, _):
            rr = pl.ds(pl.multiple_of(u * RB, RB), RB)
            h[lax.rem(k, 3), rr] = norm(y0[i, rr].astype(jnp.float32), 0)
            return 0
        lax.fori_loop(0, q // RB, body, 0)
        send_h(k)

    def add_up(j, yref, yi, rr):
        parts = []
        for t in range(NT2):
            yf = yref[yi, rr, t * TN:(t + 1) * TN].astype(jnp.float32)
            parts.append((yf + (own[lax.rem(j, 2), t, rr] + srecv[lax.rem(j, 3), t, rr].astype(jnp.float32))
                          ).astype(jnp.bfloat16))
        return jnp.concatenate(parts, axis=-1)

    def wait_sums(j):
        for t in range(NT2):
            s_copy(j, t).wait()

    def finish0(c, j, k):
        wait_sums(j)
        i = lax.rem(c, YS)
        o = lax.rem(c, 2)

        def body(u, _):
            rr = pl.ds(pl.multiple_of(u * RB, RB), RB)
            y = add_up(j, y0, i, rr)
            y1[o, rr] = y
            h[lax.rem(k, 3), rr] = norm(y.astype(jnp.float32), 1)
            return 0
        lax.fori_loop(0, q // RB, body, 0)
        send_h(k)

        @pl.when((s > 0) & (c + YS < C))
        def _():
            pl.semaphore_signal(credit, inc=1, device_id={'stage': s - 1}, device_id_type=MESH)

    def release(c):
        y_store(c).wait()

        @pl.when(s < S - 1)
        def _():
            y_next(c).wait_send()

    def finish1(c, j):
        o = lax.rem(c, 2)

        @pl.when(c >= 2)
        def _():
            release(c - 2)
        wait_sums(j)

        def body(u, _):
            rr = pl.ds(pl.multiple_of(u * RB, RB), RB)
            yout[o, rr] = add_up(j, y1, o, rr)
            return 0
        lax.fori_loop(0, q // RB, body, 0)

        @pl.when(s < S - 1)
        def _():
            @pl.when(c >= YS)
            def _():
                pl.semaphore_wait(credit, 1)
            y_next(c).start()
        y_store(c).start()

    def compute(k, b, first):
        i = lax.rem(k, 3)
        e = lax.rem(k, 2)
        ag_partner(k).wait()
        ag_cross(k).wait()
        ag_forward(k).start()
        ag_forward(k).wait_recv()
        for t in range(NT1):
            @pl.when(first)
            def _():
                w1_copy(b, t).wait()
            u = jnp.dot(h[i], w1s[b, t], preferred_element_type=jnp.float32)
            a[:, t * TN:(t + 1) * TN] = jax.nn.gelu(u).astype(jnp.bfloat16)
        ag_forward(k).wait_send()

        def combine(t):
            p_copy(k, t).wait()
            own[e, t] = own[e, t] + precv[e, t, 0:q].astype(jnp.float32)
            ssend[e, t] = (crossp[t % 2] + precv[e, t, q:2 * q].astype(jnp.float32)).astype(jnp.bfloat16)
            s_copy(k, t).start()

        for t in range(NT2):
            @pl.when(first)
            def _():
                w2_copy(b, t).wait()
            p = jnp.dot(a[...], w2s[b, t], preferred_element_type=jnp.float32)
            psend[t % 2] = p[2 * q:].astype(jnp.bfloat16)
            own[e, t] = p[0:q]
            crossp[t % 2] = p[q:2 * q]
            p_copy(k, t).start()
            if t > 0:
                combine(t - 1)
        combine(NT2 - 1)

    @pl.when(s == 0)
    def _():
        x_copy(0).start()
        x_copy(1).start()
    for b in range(NB):
        for t in range(NT1):
            w1_copy(b, t).start()
        for t in range(NT2):
            w2_copy(b, t).start()
    enter(0, 0)

    def slot(k, _):
        b = lax.rem(k, 2)
        i = lax.div(k, 2)
        c = jnp.where(b == 0, i, i - 1)

        @pl.when((c >= 0) & (c < C))
        def _():
            compute(k, b, c == 0)

        @pl.when(b == 0)
        def _():
            @pl.when((i >= 2) & (i < C + 2))
            def _():
                finish1(i - 2, k - 1)

            @pl.when(i + 1 < C)
            def _():
                enter(i + 1, k + 2)

        @pl.when((b == 1) & (i < C))
        def _():
            finish0(i, k - 1, k + 2)
        return 0

    lax.fori_loop(0, 2 * C + 3, slot, 0)
    release(C - 2)
    release(C - 1)


def solution(mesh):
    S = mesh.shape['stage']

    def local(x, g, w1, w2):
        M, TL, D = x.shape
        NB = g.shape[1]
        F = w1.shape[3]
        NQ = TL // Q
        C = M * NQ
        NT1, NT2 = F // TN, D // TN
        q = Q
        bf, f32 = jnp.bfloat16, jnp.float32
        dma, reg = pltpu.SemaphoreType.DMA, pltpu.SemaphoreType.REGULAR
        any_ = pl.BlockSpec(memory_space=pl.ANY)
        vm = pl.BlockSpec(memory_space=pltpu.VMEM)
        flops = 4 * C * NB * 4 * q * D * F
        out = pl.pallas_call(
            functools.partial(_kernel, (S, NB, C, NQ, NT1, NT2, D)),
            out_shape=jax.ShapeDtypeStruct((M, TL, D), bf),
            in_specs=[any_, vm, any_, any_],
            out_specs=any_,
            scratch_shapes=[
                pltpu.VMEM((NB, NT1, D, TN), bf),
                pltpu.VMEM((NB, NT2, F, TN), bf),
                pltpu.VMEM((3, 4 * q, D), bf),
                pltpu.VMEM((4 * q, F), bf),
                pltpu.VMEM((2, 2 * q, TN), bf),
                pltpu.VMEM((2, NT2, 2 * q, TN), bf),
                pltpu.VMEM((2, q, TN), f32),
                pltpu.VMEM((2, NT2, q, TN), f32),
                pltpu.VMEM((2, NT2, q, TN), bf),
                pltpu.VMEM((3, NT2, q, TN), bf),
                pltpu.VMEM((YS, q, D), bf),
                pltpu.VMEM((2, q, D), bf),
                pltpu.VMEM((2, q, D), bf),
                dma((2, NB, max(NT1, NT2))),
                dma((3,)), dma((3,)), dma((3,)), dma((3, 3)),
                dma((2,)), dma((2, NT2)), dma((2, NT2)), dma((3, NT2)),
                dma((YS,)), dma((2,)), dma((2,)), reg,
            ],
            compiler_params=pltpu.CompilerParams(
                has_side_effects=True, vmem_limit_bytes=67043328),
            cost_estimate=pl.CostEstimate(flops=flops, bytes_accessed=2 * (2 * M * TL * D + 2 * NB * D * F),
                                          transcendentals=C * NB * 4 * q * F),
            name='stages',
        )(x, g[0].astype(f32)[:, None, :], w1[0], w2[0])
        return out[None]

    return jax.shard_map(
        local, mesh=mesh,
        in_specs=(P(None, 'tp', None), P('stage', None, None),
                  P('stage', None, None, 'tp'), P('stage', None, 'tp', None)),
        out_specs=P('stage', None, 'tp', None), check_vma=False)
```

```python
import functools

import jax
import jax.numpy as jnp
from jax import lax
from jax.experimental import pallas as pl
from jax.experimental.pallas import tpu as pltpu
from jax.sharding import PartitionSpec as P

EPS = 1e-5
Q = 32
TN = 512
YS = 4
RS = 4
RB = 16
MESH = pl.DeviceIdType.MESH


def _kernel(cfg, x_hbm, g_ref, w1_hbm, w2_hbm, y_hbm, xc_hbm,
            w1s, w2s, h, a, psend, precv, keep, ssend, srecv, y0, y1, yout,
            w_sem, h_send, h_recv, p_send, p_recv, s_send, s_recv,
            yin_sem, ysend_sem, yhbm_sem, xs_send, xs_recv, credit):
    S, NB, C, NQ, NT1, NT2, D = cfg
    q = Q
    s = lax.axis_index('stage')
    r = lax.axis_index('tp')
    xr = lax.div(r, 2)
    cr = lax.rem(r, 2)
    partner = xr * 2 + (1 - cr)
    cross = (1 - xr) * 2 + cr
    first_stage, last_stage = s == 0, s == S - 1


    def w1_copy(b, t):
        return pltpu.make_async_copy(w1_hbm.at[b, :, pl.ds(t * TN, TN)], w1s.at[b, t], w_sem.at[0, b, t])

    def w2_copy(b, t):
        return pltpu.make_async_copy(w2_hbm.at[b, :, pl.ds(t * TN, TN)], w2s.at[b, t], w_sem.at[1, b, t])

    def remote(src, dst, ss, rs, **dev):
        return pltpu.make_async_remote_copy(src_ref=src, dst_ref=dst, send_sem=ss, recv_sem=rs,
                                            device_id=dev, device_id_type=MESH)

    def h_copy(b):
        return remote(h.at[b, pl.ds(0, 2 * q)], h.at[b, pl.ds(2 * q, 2 * q)],
                      h_send.at[b], h_recv.at[b], tp=partner)

    def p_copy(b, t):
        return remote(psend.at[t % 2], precv.at[b, t], p_send.at[t % 2], p_recv.at[b, t], tp=partner)

    def s_copy(b, c, t):
        e, i, k = lax.rem(c, 2), lax.rem(c, RS), (2 - b) * q
        return remote(ssend.at[b, e, t, pl.ds(0, k)], srecv.at[b, i, t, pl.ds(0, k)],
                      s_send.at[b, e, t], s_recv.at[b, i, t], tp=cross)

    def hbm_rows(ref, c):
        return ref.at[lax.div(c, NQ), pl.ds(pl.multiple_of(lax.rem(c, NQ) * q, q), q)]

    def x_send(c):
        return pltpu.make_async_remote_copy(
            src_ref=hbm_rows(x_hbm, c), dst_ref=hbm_rows(xc_hbm, c),
            send_sem=xs_send.at[c], recv_sem=xs_recv.at[c],
            device_id={'stage': jnp.int32(0), 'tp': cross}, device_id_type=MESH)

    def x_copy(c, part):
        i = lax.rem(c, YS)
        src = x_hbm if part == 0 else xc_hbm
        return pltpu.make_async_copy(hbm_rows(src, c), y0.at[i, pl.ds(part * q, q)], yin_sem.at[i, part])

    def y_next(c, part):
        i, o = lax.rem(c, YS), lax.rem(c, 2)
        return remote(yout.at[o], y0.at[i, pl.ds(part * q, q)], ysend_sem.at[o, part], yin_sem.at[i, part],
                      stage=s + 1, tp=r if part == 0 else cross)

    def y_store(c):
        o = lax.rem(c, 2)
        return pltpu.make_async_copy(yout.at[o], hbm_rows(y_hbm, c), yhbm_sem.at[o])

    def norm(yf, b):
        mu = jnp.mean(yf, axis=-1, keepdims=True)
        d = yf - mu
        var = jnp.mean(jnp.square(d), axis=-1, keepdims=True)
        return (d * lax.rsqrt(var + EPS) * g_ref[b]).astype(jnp.bfloat16)

    def fetch(c):
        x_send(c).wait_recv()
        x_copy(c, 0).start()
        x_copy(c, 1).start()

    def enter(c):
        i = lax.rem(c, YS)

        @pl.when(first_stage)
        def _():
            x_copy(c, 0).wait()
            x_copy(c, 1).wait()

            @pl.when(c + 2 < C)
            def _():
                fetch(c + 2)

        @pl.when(jnp.logical_not(first_stage))
        def _():
            y_next(c, 0).wait_recv()
            y_next(c, 1).wait_recv()

        for u in range(2 * q // RB):
            rr = slice(u * RB, (u + 1) * RB)
            h[0, rr] = norm(y0[i, rr].astype(jnp.float32), 0)
        h_copy(0).start()

    def add_up(y, b, c, lo):
        e, i = lax.rem(c, 2), lax.rem(c, RS)
        mine = slice((lo + q) % (2 * q), (lo + q) % (2 * q) + RB)
        theirs = slice(lo, lo + RB)
        parts = []
        for t in range(NT2):
            parts.append((y[:, t * TN:(t + 1) * TN].astype(jnp.float32)
                          + (ssend[b, e, t, mine].astype(jnp.float32)
                             + srecv[b, i, t, theirs].astype(jnp.float32))).astype(jnp.bfloat16))
        return jnp.concatenate(parts, axis=-1)

    def finish0(c):
        for t in range(NT2):
            s_copy(0, c, t).wait()
        i, o = lax.rem(c, YS), lax.rem(c, 2)
        for u in range(2 * q // RB):
            rr = slice(u * RB, (u + 1) * RB)
            y = add_up(y0[i, rr], 0, c, u * RB)
            if u * RB < q:
                y1[o, rr] = y
            h[1, rr] = norm(y.astype(jnp.float32), 1)
        h_copy(1).start()

        @pl.when((s > 0) & (c + YS < C))
        def _():
            pl.semaphore_signal(credit.at[0], inc=1, device_id={'stage': s - 1, 'tp': r}, device_id_type=MESH)
            pl.semaphore_signal(credit.at[1], inc=1, device_id={'stage': s - 1, 'tp': cross},
                                device_id_type=MESH)

    def release(c):
        y_store(c).wait()

        @pl.when(s < S - 1)
        def _():
            y_next(c, 1).wait_send()
            y_next(c, 0).wait_send()

    def finish1(c):
        o = lax.rem(c, 2)

        @pl.when(c >= 2)
        def _():
            release(c - 2)
        for t in range(NT2):
            s_copy(1, c, t).wait()
        for u in range(q // RB):
            rr = slice(u * RB, (u + 1) * RB)
            yout[o, rr] = add_up(y1[o, rr], 1, c, u * RB)

        @pl.when(s < S - 1)
        def _():
            @pl.when(c >= YS)
            def _():
                pl.semaphore_wait(credit.at[0], 1)
                pl.semaphore_wait(credit.at[1], 1)
            y_next(c, 1).start()
            y_next(c, 0).start()
        y_store(c).start()

    def combine(b, c, t):
        e = lax.rem(c, 2)
        p_copy(b, t).wait()
        ssend[b, e, t, 0:q] = (keep[t % 2, q:2 * q] + precv[b, t, q:2 * q].astype(jnp.float32)
                               ).astype(jnp.bfloat16)
        ssend[b, e, t, q:2 * q] = (keep[t % 2, 0:q] + precv[b, t, 0:q].astype(jnp.float32)
                                   ).astype(jnp.bfloat16)
        s_copy(b, c, t).start()

    def compute(b, c):
        @pl.when(c == 0)
        def _():
            for t in range(NT1):
                w1_copy(b, t).wait()
        h_copy(b).wait()
        for t in range(NT1):
            u = jnp.dot(h[b], w1s[b, t], preferred_element_type=jnp.float32)
            a[:, t * TN:(t + 1) * TN] = jax.nn.gelu(u).astype(jnp.bfloat16)

        @pl.when(c == 0)
        def _():
            for t in range(NT2):
                w2_copy(b, t).wait()
        for t in range(NT2):
            p = jnp.dot(a[...], w2s[b, t], preferred_element_type=jnp.float32)
            psend[t % 2] = p[2 * q:].astype(jnp.bfloat16)
            keep[t % 2] = p[0:2 * q]
            p_copy(b, t).start()
            if t > 0:
                combine(b, c, t - 1)

    @pl.when(last_stage)
    def _():
        def send(c, _):
            x_send(c).start()
            return 0
        lax.fori_loop(0, C, send, 0)

    for b in range(NB):
        for t in range(NT1):
            w1_copy(b, t).start()
        for t in range(NT2):
            w2_copy(b, t).start()

    @pl.when(first_stage)
    def _():
        fetch(0)
        fetch(1)
    enter(0)

    def step(i, _):
        @pl.when(i < C)
        def _():
            compute(0, i)

        @pl.when((i >= 1) & (i <= C))
        def _():
            finish0(i - 1)

        @pl.when(i >= 2)
        def _():
            finish1(i - 2)

        @pl.when(i < C)
        def _():
            combine(0, i, NT2 - 1)

        @pl.when((i >= 1) & (i <= C))
        def _():
            compute(1, i - 1)

        @pl.when(i + 1 < C)
        def _():
            enter(i + 1)

        @pl.when((i >= 1) & (i <= C))
        def _():
            combine(1, i - 1, NT2 - 1)
        return 0

    lax.fori_loop(0, C + 2, step, 0)
    release(C - 2)
    release(C - 1)

    @pl.when(last_stage)
    def _():
        def sent(c, _):
            x_send(c).wait_send()
            return 0
        lax.fori_loop(0, C, sent, 0)


def solution(mesh):
    S = mesh.shape['stage']

    def local(x, g, w1, w2):
        M, TL, D = x.shape
        NB = g.shape[1]
        F = w1.shape[3]
        NQ = TL // Q
        C = M * NQ
        NT1, NT2 = F // TN, D // TN
        q = Q
        bf, f32 = jnp.bfloat16, jnp.float32
        dma, reg = pltpu.SemaphoreType.DMA, pltpu.SemaphoreType.REGULAR
        any_ = pl.BlockSpec(memory_space=pl.ANY)
        vm = pl.BlockSpec(memory_space=pltpu.VMEM)
        flops = 4 * C * NB * 4 * q * D * F
        out, _ = pl.pallas_call(
            functools.partial(_kernel, (S, NB, C, NQ, NT1, NT2, D)),
            out_shape=(jax.ShapeDtypeStruct((M, TL, D), bf), jax.ShapeDtypeStruct((M, TL, D), bf)),
            in_specs=[any_, vm, any_, any_],
            out_specs=(any_, any_),
            scratch_shapes=[
                pltpu.VMEM((NB, NT1, D, TN), bf),
                pltpu.VMEM((NB, NT2, F, TN), bf),
                pltpu.VMEM((NB, 4 * q, D), bf),
                pltpu.VMEM((4 * q, F), bf),
                pltpu.VMEM((2, 2 * q, TN), bf),
                pltpu.VMEM((NB, NT2, 2 * q, TN), bf),
                pltpu.VMEM((2, 2 * q, TN), f32),
                pltpu.VMEM((NB, 2, NT2, 2 * q, TN), bf),
                pltpu.VMEM((NB, RS, NT2, 2 * q, TN), bf),
                pltpu.VMEM((YS, 2 * q, D), bf),
                pltpu.VMEM((2, q, D), bf),
                pltpu.VMEM((2, q, D), bf),
                dma((2, NB, max(NT1, NT2))),
                dma((NB,)), dma((NB,)),
                dma((2,)), dma((NB, NT2)), dma((NB, 2, NT2)), dma((NB, RS, NT2)),
                dma((YS, 2)), dma((2, 2)), dma((2,)), dma((C,)), dma((C,)), reg((2,)),
            ],
            compiler_params=pltpu.CompilerParams(
                has_side_effects=True, vmem_limit_bytes=67043328),
            cost_estimate=pl.CostEstimate(flops=flops, bytes_accessed=2 * (2 * M * TL * D + 2 * NB * D * F),
                                          transcendentals=C * NB * 4 * q * F),
            name='stages',
        )(x, g[0].astype(f32)[:, None, :], w1[0], w2[0])
        return out[None]

    return jax.shard_map(
        local, mesh=mesh,
        in_specs=(P(None, 'tp', None), P('stage', None, None),
                  P('stage', None, None, 'tp'), P('stage', None, 'tp', None)),
        out_specs=P('stage', None, 'tp', None), check_vma=False)
```

```python
import functools

import jax
import jax.numpy as jnp
from jax import lax
from jax.experimental import pallas as pl
from jax.experimental.pallas import tpu as pltpu
from jax.sharding import PartitionSpec as P

EPS = 1e-5
Q = 32
TN = 512
YS = 4
RS = 4
T0 = 3
RB = 16
MESH = pl.DeviceIdType.MESH


def _kernel(cfg, x_hbm, g_ref, w1_hbm, w2_hbm, y_hbm, xc_hbm,
            w1s, w2s, h, a, psend, precv, keep, ssend, srecv, y0, y1, yout,
            w_sem, h_send, h_recv, p_send, p_recv, s_send, s_recv,
            yin_sem, ysend_sem, yhbm_sem, xs_send, xs_recv, credit):
    S, NB, C, NQ, NT1, NT2, D = cfg
    q = Q
    s = lax.axis_index('stage')
    r = lax.axis_index('tp')
    xr = lax.div(r, 2)
    cr = lax.rem(r, 2)
    partner = xr * 2 + (1 - cr)
    cross = (1 - xr) * 2 + cr
    first_stage = s == 0


    def w1_copy(b, t):
        return pltpu.make_async_copy(w1_hbm.at[b, :, pl.ds(t * TN, TN)], w1s.at[b, t], w_sem.at[0, b, t])

    def w2_copy(b, t):
        return pltpu.make_async_copy(w2_hbm.at[b, :, pl.ds(t * TN, TN)], w2s.at[b, t], w_sem.at[1, b, t])

    def remote(src, dst, ss, rs, **dev):
        return pltpu.make_async_remote_copy(src_ref=src, dst_ref=dst, send_sem=ss, recv_sem=rs,
                                            device_id=dev, device_id_type=MESH)

    def h_copy(b):
        return remote(h.at[b, pl.ds(0, 2 * q)], h.at[b, pl.ds(2 * q, 2 * q)],
                      h_send.at[b], h_recv.at[b], tp=partner)

    def p_copy(b, t):
        return remote(psend.at[t], precv.at[b, t], p_send.at[t], p_recv.at[b, t], tp=partner)

    def s_copy(b, c, t):
        e, i, k = lax.rem(c, 2), lax.rem(c, RS), (2 - b) * q
        return remote(ssend.at[b, e, t, pl.ds(0, k)], srecv.at[b, i, t, pl.ds(0, k)],
                      s_send.at[b, e, t], s_recv.at[b, i, t], tp=cross)

    def hbm_rows(ref, c):
        return ref.at[lax.div(c, NQ), pl.ds(pl.multiple_of(lax.rem(c, NQ) * q, q), q)]

    def x_send(c):
        return pltpu.make_async_remote_copy(
            src_ref=hbm_rows(x_hbm, c), dst_ref=hbm_rows(xc_hbm, c),
            send_sem=xs_send.at[c], recv_sem=xs_recv.at[c],
            device_id={'stage': jnp.int32(0), 'tp': cross}, device_id_type=MESH)

    def x_copy(c, part):
        i = lax.rem(c, YS)
        src = x_hbm if part == 0 else xc_hbm
        return pltpu.make_async_copy(hbm_rows(src, c), y0.at[i, pl.ds(part * q, q)], yin_sem.at[i, part])

    def y_next(c, part):
        i, o = lax.rem(c, YS), lax.rem(c, 2)
        return remote(yout.at[o], y0.at[i, pl.ds(part * q, q)], ysend_sem.at[o, part], yin_sem.at[i, part],
                      stage=s + 1, tp=r if part == 0 else cross)

    def y_store(c):
        o = lax.rem(c, 2)
        return pltpu.make_async_copy(yout.at[o], hbm_rows(y_hbm, c), yhbm_sem.at[o])

    def norm(yf, b):
        mu = jnp.mean(yf, axis=-1, keepdims=True)
        d = yf - mu
        var = jnp.mean(jnp.square(d), axis=-1, keepdims=True)
        return (d * lax.rsqrt(var + EPS) * g_ref[b]).astype(jnp.bfloat16)

    def fetch(c):
        x_send(c).wait_recv()
        x_copy(c, 0).start()
        x_copy(c, 1).start()

    def enter(c):
        i = lax.rem(c, YS)

        @pl.when(first_stage)
        def _():
            x_copy(c, 0).wait()
            x_copy(c, 1).wait()

            @pl.when(c + 2 < C)
            def _():
                fetch(c + 2)

        @pl.when(jnp.logical_not(first_stage))
        def _():
            y_next(c, 0).wait_recv()
            y_next(c, 1).wait_recv()

        for u in range(2 * q // RB):
            rr = slice(u * RB, (u + 1) * RB)
            h[0, rr] = norm(y0[i, rr].astype(jnp.float32), 0)
        h_copy(0).start()

    def add_up(y, b, c, lo):
        e, i = lax.rem(c, 2), lax.rem(c, RS)
        mine = slice((lo + q) % (2 * q), (lo + q) % (2 * q) + RB)
        theirs = slice(lo, lo + RB)
        parts = []
        for t in range(NT2):
            parts.append((y[:, t * TN:(t + 1) * TN].astype(jnp.float32)
                          + (ssend[b, e, t, mine].astype(jnp.float32)
                             + srecv[b, i, t, theirs].astype(jnp.float32))).astype(jnp.bfloat16))
        return jnp.concatenate(parts, axis=-1)

    def finish0(c):
        for t in range(NT2):
            s_copy(0, c, t).wait()
        i, o = lax.rem(c, YS), lax.rem(c, 2)
        for u in range(2 * q // RB):
            rr = slice(u * RB, (u + 1) * RB)
            y = add_up(y0[i, rr], 0, c, u * RB)
            if u * RB < q:
                y1[o, rr] = y
            h[1, rr] = norm(y.astype(jnp.float32), 1)
        h_copy(1).start()

        @pl.when((s > 0) & (c + YS < C))
        def _():
            pl.semaphore_signal(credit.at[0], inc=1, device_id={'stage': s - 1, 'tp': r}, device_id_type=MESH)
            pl.semaphore_signal(credit.at[1], inc=1, device_id={'stage': s - 1, 'tp': cross},
                                device_id_type=MESH)

    def release(c):
        y_store(c).wait()

        @pl.when(s < S - 1)
        def _():
            y_next(c, 1).wait_send()
            y_next(c, 0).wait_send()

    def finish1(c):
        o = lax.rem(c, 2)

        @pl.when(c >= 2)
        def _():
            release(c - 2)
        for t in range(NT2):
            s_copy(1, c, t).wait()
        for u in range(q // RB):
            rr = slice(u * RB, (u + 1) * RB)
            yout[o, rr] = add_up(y1[o, rr], 1, c, u * RB)

        @pl.when(s < S - 1)
        def _():
            @pl.when(c >= YS)
            def _():
                pl.semaphore_wait(credit.at[0], 1)
                pl.semaphore_wait(credit.at[1], 1)
            y_next(c, 1).start()
            y_next(c, 0).start()
        y_store(c).start()

    def combine(b, c, t):
        e = lax.rem(c, 2)
        p_copy(b, t).wait()
        ssend[b, e, t, 0:q] = (keep[t, q:2 * q] + precv[b, t, q:2 * q].astype(jnp.float32)
                               ).astype(jnp.bfloat16)
        ssend[b, e, t, q:2 * q] = (keep[t, 0:q] + precv[b, t, 0:q].astype(jnp.float32)
                                   ).astype(jnp.bfloat16)
        s_copy(b, c, t).start()

    def compute(b, c):
        @pl.when(c == 0)
        def _():
            for t in range(NT1):
                w1_copy(b, t).wait()
        h_copy(b).wait()
        for t in range(NT1):
            u = jnp.dot(h[b], w1s[b, t], preferred_element_type=jnp.float32)
            a[:, t * TN:(t + 1) * TN] = jax.nn.gelu(u).astype(jnp.bfloat16)

        @pl.when(c == 0)
        def _():
            for t in range(NT2):
                w2_copy(b, t).wait()
        for t in range(NT2):
            p = jnp.dot(a[...], w2s[b, t], preferred_element_type=jnp.float32)
            psend[t] = p[2 * q:].astype(jnp.bfloat16)
            keep[t] = p[0:2 * q]
            if t == T0 - 1:
                for v in range(T0):
                    p_copy(b, v).start()
        for v in range(T0, NT2):
            p_copy(b, v).start()
        for v in range(T0):
            combine(b, c, v)

    def x_mine(c):
        src = jnp.where(c < 36, 1 + lax.rem(c, 3), jnp.where(lax.rem(c - 36, 14) < 5, 2, 3))
        return s == src

    def send(c, _):
        @pl.when(x_mine(c))
        def _():
            x_send(c).start()
        return 0
    lax.fori_loop(0, C, send, 0)

    for b in range(NB):
        for t in range(NT1):
            w1_copy(b, t).start()
        for t in range(NT2):
            w2_copy(b, t).start()

    @pl.when(first_stage)
    def _():
        fetch(0)
        fetch(1)
    enter(0)

    def step(i, _):
        @pl.when(i < C)
        def _():
            compute(0, i)

        @pl.when((i >= 1) & (i <= C))
        def _():
            finish0(i - 1)

        @pl.when(i >= 2)
        def _():
            finish1(i - 2)

        @pl.when(i < C)
        def _():
            for t in range(T0, NT2):
                combine(0, i, t)

        @pl.when((i >= 1) & (i <= C))
        def _():
            compute(1, i - 1)

        @pl.when(i + 1 < C)
        def _():
            enter(i + 1)

        @pl.when((i >= 1) & (i <= C))
        def _():
            for t in range(T0, NT2):
                combine(1, i - 1, t)
        return 0

    lax.fori_loop(0, C + 2, step, 0)
    release(C - 2)
    release(C - 1)

    def sent(c, _):
        @pl.when(x_mine(c))
        def _():
            x_send(c).wait_send()
        return 0
    lax.fori_loop(0, C, sent, 0)


def solution(mesh):
    S = mesh.shape['stage']

    def local(x, g, w1, w2):
        M, TL, D = x.shape
        NB = g.shape[1]
        F = w1.shape[3]
        NQ = TL // Q
        C = M * NQ
        NT1, NT2 = F // TN, D // TN
        q = Q
        bf, f32 = jnp.bfloat16, jnp.float32
        dma, reg = pltpu.SemaphoreType.DMA, pltpu.SemaphoreType.REGULAR
        any_ = pl.BlockSpec(memory_space=pl.ANY)
        vm = pl.BlockSpec(memory_space=pltpu.VMEM)
        flops = 4 * C * NB * 4 * q * D * F
        out, _ = pl.pallas_call(
            functools.partial(_kernel, (S, NB, C, NQ, NT1, NT2, D)),
            out_shape=(jax.ShapeDtypeStruct((M, TL, D), bf), jax.ShapeDtypeStruct((M, TL, D), bf)),
            in_specs=[any_, vm, any_, any_],
            out_specs=(any_, any_),
            scratch_shapes=[
                pltpu.VMEM((NB, NT1, D, TN), bf),
                pltpu.VMEM((NB, NT2, F, TN), bf),
                pltpu.VMEM((NB, 4 * q, D), bf),
                pltpu.VMEM((4 * q, F), bf),
                pltpu.VMEM((NT2, 2 * q, TN), bf),
                pltpu.VMEM((NB, NT2, 2 * q, TN), bf),
                pltpu.VMEM((NT2, 2 * q, TN), f32),
                pltpu.VMEM((NB, 2, NT2, 2 * q, TN), bf),
                pltpu.VMEM((NB, RS, NT2, 2 * q, TN), bf),
                pltpu.VMEM((YS, 2 * q, D), bf),
                pltpu.VMEM((2, q, D), bf),
                pltpu.VMEM((2, q, D), bf),
                dma((2, NB, max(NT1, NT2))),
                dma((NB,)), dma((NB,)),
                dma((NT2,)), dma((NB, NT2)), dma((NB, 2, NT2)), dma((NB, RS, NT2)),
                dma((YS, 2)), dma((2, 2)), dma((2,)), dma((C,)), dma((C,)), reg((2,)),
            ],
            compiler_params=pltpu.CompilerParams(
                has_side_effects=True, vmem_limit_bytes=67043328),
            cost_estimate=pl.CostEstimate(flops=flops, bytes_accessed=2 * (2 * M * TL * D + 2 * NB * D * F),
                                          transcendentals=C * NB * 4 * q * F),
            name='stages',
        )(x, g[0].astype(f32)[:, None, :], w1[0], w2[0])
        return out[None]

    return jax.shard_map(
        local, mesh=mesh,
        in_specs=(P(None, 'tp', None), P('stage', None, None),
                  P('stage', None, None, 'tp'), P('stage', None, 'tp', None)),
        out_specs=P('stage', None, 'tp', None), check_vma=False)
```
